32 devices in a mesh: ha: 2 (over y), wa: 16 (over z, x, core).
Axes of the slice: x: 2, y: 2, z: 4, core: 2. Of those that a mesh axis runs over, the one named last changes fastest.
Arguments:
- query_field: float32 [2, 32, 64, 256], P(None, 'ha', 'wa'), may hold values from -150 to 150, as said below
- key_field: float32 [2, 32, 64, 256], P(None, 'ha', 'wa'), may hold values from -6 to 6
- value_field: float32 [2, 32, 64, 256], P(None, 'ha', 'wa'), may hold values from -6 to 6
- output_grad: float32 [2, 32, 64, 256], P(None, 'ha', 'wa'), may hold values from -6 to 6
Outputs:
- query_grad: float32 [2, 32, 64, 256], P(None, 'ha', 'wa')
- key_grad: float32 [2, 32, 64, 256], P(None, 'ha', 'wa')
- value_grad: float32 [2, 32, 64, 256], P(None, 'ha', 'wa')
The draws below stay inside these ranges and needn't reach their ends.
Inputs may be any that keep to these rules, and one draw needn't show every extreme that they name: `query_field`: queries and keys are real-valued with no structure promised.
All inputs are finite; a program needn't handle non-finite values.
Results may differ from the reference program's by a relative error of at most 0.0003.
Values sent between devices are 32-bit elements; how exact they have to be, the bound alone decides.
No kernel may reach another device: no remote copies, remote signals or barrier semaphores. Data moves between devices by JAX's collectives and lax.ppermute only.
A program may use at most 128 MiB of HBM per device.

```python
import jax
import jax.numpy as jnp
from jax import lax

FRAMES = 2
HEADS = 2
HEAD_DIM = 128
TILE = 16
CHANNELS = 256
HEIGHT = 32
WIDTH = 64


def draw_common(base):
    shape = (FRAMES, HEIGHT, WIDTH, CHANNELS)
    key_base = jnp.clip(jax.random.normal(jax.random.fold_in(base, 11), shape, jnp.float32), -6.0, 6.0)
    query_base = jnp.clip(jax.random.normal(jax.random.fold_in(base, 12), shape, jnp.float32), -6.0, 6.0)
    return (query_base, key_base)


def draw_query_field(key, part):
    return draw_common(jax.random.fold_in(key, 5))[0]


def draw_key_field(key, part):
    return draw_common(jax.random.fold_in(key, 5))[1]


def shard_levels(own_key, extent, shards, least, largest):
    level, own = 1.0, jax.random.fold_in(own_key, 6)
    for position, parts in shards:
        draws = jnp.exp(jax.random.uniform(jax.random.fold_in(own, position), (parts,), jnp.float32, least / len(shards), largest / len(shards)))
        level = level * jnp.repeat(draws, extent[position] // parts).reshape([-1 if axis == position else 1 for axis in range(len(extent))])
    return level


def bell_draw(key, dims, scale, reach, shards=(), held_as=jnp.bfloat16):
    values = scale * jax.random.normal(key, dims, jnp.float32)
    if shards:
        values = values * shard_levels(key, dims, shards, -0.22, 0.18)
    return jnp.clip(values, -reach, reach).astype(held_as)


def setup_inputs(seed: int = 0) -> dict:
    seeds = jax.random.split(jax.random.key(seed), 5)
    return {
        "query_field": draw_query_field(jax.random.fold_in(seeds[4], 71), 0),
        "key_field": draw_key_field(jax.random.fold_in(seeds[4], 71), 0),
        "value_field": bell_draw(seeds[2], (FRAMES, HEIGHT, WIDTH, CHANNELS), 1.0, 6.0, ((1, 2), (2, 16)), jnp.float32),
        "output_grad": bell_draw(seeds[3], (FRAMES, HEIGHT, WIDTH, CHANNELS), 1.0, 6.0, ((1, 2), (2, 16)), jnp.float32),
    }


def tile_grads(query_rows, grad_rows, key_rows, value_rows, key_valid):
    score_scale = HEAD_DIM ** -0.5
    highest = lax.Precision.HIGHEST
    mask_bias = jnp.where(key_valid, jnp.float32(0.0), jnp.float32(-1e30))
    query_parts = []
    key_parts = []
    value_parts = []
    for head_index in range(HEADS):
        head_start = head_index * HEAD_DIM
        head_stop = head_start + HEAD_DIM
        query_scaled = query_rows[:, head_start:head_stop] * score_scale
        grad_head = grad_rows[:, head_start:head_stop]
        key_head = key_rows[:, head_start:head_stop]
        value_head = value_rows[:, head_start:head_stop]
        scores = jnp.dot(query_scaled, key_head.T, precision=highest) + mask_bias[None, :]
        row_peak = jnp.max(scores, axis=1, keepdims=True)
        weights = jnp.exp(scores - row_peak)
        inverse = 1.0 / jnp.sum(weights, axis=1, keepdims=True)
        probabilities = weights * inverse
        dprobs = jnp.dot(grad_head, value_head.T, precision=highest)
        center = jnp.sum(probabilities * dprobs, axis=1, keepdims=True)
        dscores = probabilities * (dprobs - center)
        query_parts.append(jnp.dot(dscores, key_head, precision=highest) * score_scale)
        key_parts.append(jnp.dot(dscores.T, query_scaled, precision=highest))
        value_parts.append(jnp.dot(probabilities.T, grad_head, precision=highest))
    return (jnp.concatenate(query_parts, axis=1), jnp.concatenate(key_parts, axis=1),
            jnp.concatenate(value_parts, axis=1))


def reference(query_field, key_field, value_field, output_grad):
    tiles_high = HEIGHT // TILE
    tiles_wide = WIDTH // TILE
    padding = ((0, 0), (TILE, TILE), (TILE, TILE), (0, 0))
    key_padded = jnp.pad(key_field, padding)
    value_padded = jnp.pad(value_field, padding)
    window_span = jnp.arange(3 * TILE, dtype=jnp.int32)
    window_shape = (FRAMES, 3 * TILE, 3 * TILE, CHANNELS)

    def visit(carry, tile_number):
        key_acc, value_acc = carry
        tile_row = tile_number // tiles_wide
        tile_col = tile_number % tiles_wide
        row_start = (tile_row * TILE).astype(jnp.int32)
        col_start = (tile_col * TILE).astype(jnp.int32)
        anchor = jnp.int32(0)
        where_tile = (anchor, row_start, col_start, anchor)
        query_rows = lax.dynamic_slice(query_field, where_tile, (FRAMES, TILE, TILE, CHANNELS)).reshape(-1, CHANNELS)
        grad_rows = lax.dynamic_slice(output_grad, where_tile, (FRAMES, TILE, TILE, CHANNELS)).reshape(-1, CHANNELS)
        key_rows = lax.dynamic_slice(key_padded, where_tile, window_shape).reshape(-1, CHANNELS)
        value_rows = lax.dynamic_slice(value_padded, where_tile, window_shape).reshape(-1, CHANNELS)
        rows_global = row_start - TILE + window_span
        cols_global = col_start - TILE + window_span
        row_ok = (rows_global >= 0) & (rows_global < HEIGHT)
        col_ok = (cols_global >= 0) & (cols_global < WIDTH)
        plane_ok = row_ok[:, None] & col_ok[None, :]
        key_valid = jnp.broadcast_to(plane_ok[None], (FRAMES, 3 * TILE, 3 * TILE)).reshape(-1)
        query_part, key_part, value_part = tile_grads(query_rows, grad_rows, key_rows, value_rows, key_valid)
        key_acc = lax.dynamic_update_slice(
            key_acc, lax.dynamic_slice(key_acc, where_tile, window_shape) + key_part.reshape(window_shape), where_tile)
        value_acc = lax.dynamic_update_slice(
            value_acc, lax.dynamic_slice(value_acc, where_tile, window_shape) + value_part.reshape(window_shape), where_tile)
        return (key_acc, value_acc), query_part.reshape(FRAMES, TILE, TILE, CHANNELS)

    empty = jnp.zeros(key_padded.shape, jnp.float32)
    numbers = jnp.arange(tiles_high * tiles_wide, dtype=jnp.int32)
    (key_acc, value_acc), query_tiles = lax.scan(visit, (empty, empty), numbers)
    query_grad = query_tiles.reshape(tiles_high, tiles_wide, FRAMES, TILE, TILE, CHANNELS)
    query_grad = query_grad.transpose(2, 0, 3, 1, 4, 5).reshape(FRAMES, HEIGHT, WIDTH, CHANNELS)
    key_grad = key_acc[:, TILE:TILE + HEIGHT, TILE:TILE + WIDTH]
    value_grad = value_acc[:, TILE:TILE + HEIGHT, TILE:TILE + WIDTH]
    return query_grad, key_grad, value_grad
```

```python
import functools

import jax
import jax.numpy as jnp
from jax import lax
from jax.experimental import pallas as pl
from jax.experimental.pallas import tpu as pltpu
from jax.sharding import PartitionSpec as P

HEADS = 2
HEAD_DIM = 128
TILE = 16
AXES = ("ha", "wa")
SCORE_SCALE = HEAD_DIM ** (-0.5)
F32 = jnp.float32
BF16 = jnp.bfloat16


def split2(x):
    high = x.astype(BF16)
    return high, (x - high.astype(F32)).astype(BF16)


def split3(x):
    high = x.astype(BF16)
    rest = x - high.astype(F32)
    mid = rest.astype(BF16)
    return high, mid, (rest - mid.astype(F32)).astype(BF16)


def nt_dot(a, b):
    return lax.dot_general(a, b, (((1,), (1,)), ((), ())), preferred_element_type=F32)


def nn_dot(a, b):
    return lax.dot_general(a, b, (((1,), (0,)), ((), ())), preferred_element_type=F32)


def flat_rows(ref, part):
    block = ref[:, part]
    return block.reshape(-1, block.shape[-1])


def score_kernel(nq, nk, *refs):
    bias = refs[0]
    qd = refs[1 : 1 + nq]
    kv = refs[1 + nq : 1 + nq + nk]
    weights, dprobs, stats = refs[1 + nq + nk : 4 + nq + nk]
    key_cat, value_cat = refs[4 + nq + nk :]
    rows = weights.shape[1] // nk
    for b in range(nk):
        k1, k2, k3 = split3(flat_rows(kv[b], 0))
        key_cat[b * rows : (b + 1) * rows] = jnp.concatenate([k1, k1, k2, k2, k1, k3], axis=1)
        v1, v2 = split2(flat_rows(kv[b], 1))
        value_cat[b * rows : (b + 1) * rows] = jnp.concatenate([v1, v1, v2, v2], axis=1)
    for i in range(nq):
        q1, q2, q3 = split3(flat_rows(qd[i], 0))
        query_cat = jnp.concatenate([q1, q2, q1, q2, q3, q1], axis=1)
        d1, d2 = split2(flat_rows(qd[i], 1))
        grad_cat = jnp.concatenate([d1, d2, d1, d2], axis=1)
        peak = None
        for b in range(nk):
            part = slice(b * rows, (b + 1) * rows)
            scores = nt_dot(key_cat[part], query_cat) + bias[b]
            weights[i, part] = scores
            top = jnp.max(scores, axis=0, keepdims=True)
            peak = top if peak is None else jnp.maximum(peak, top)
        total = jnp.zeros_like(peak)
        center = jnp.zeros_like(peak)
        for b in range(nk):
            part = slice(b * rows, (b + 1) * rows)
            w = jnp.exp(weights[i, part] - peak)
            dp = nt_dot(value_cat[part], grad_cat)
            weights[i, part] = w
            dprobs[i, part] = dp
            total += jnp.sum(w, axis=0, keepdims=True)
            center += jnp.sum(w * dp, axis=0, keepdims=True)
        stats[i] = jnp.concatenate([peak, total, center, jnp.zeros((5, peak.shape[1]), F32)], axis=0)


def grad_kernel(nq, nk, *refs):
    weights, dprobs, coef = refs[:3]
    qd = refs[3 : 3 + nq]
    kv = refs[3 + nq : 3 + nq + nk]
    outs = refs[3 + nq + nk :]
    query_out = outs[:nq]
    kv_out = outs[nq : nq + nk]
    key_acc, value_acc, key_t = outs[nq + nk :]
    rows = weights.shape[1] // nk
    for b in range(nk):
        k1, k2 = split2(flat_rows(kv[b], 0).T)
        both = jnp.concatenate([k1, k2], axis=0)
        key_t[b] = jnp.concatenate([both, both], axis=1)
    for i in range(nq):
        q1, q2 = split2(flat_rows(qd[i], 0))
        query_pair = jnp.concatenate([q1, q2], axis=1)
        query_pair = jnp.concatenate([query_pair, query_pair], axis=0)
        d1, d2 = split2(flat_rows(qd[i], 1))
        grad_pair = jnp.concatenate([d1, d2], axis=1)
        grad_pair = jnp.concatenate([grad_pair, grad_pair], axis=0)
        scale = coef[i, 0:1]
        center = coef[i, 1:2]
        query_sum = None
        for b in range(nk):
            part = slice(b * rows, (b + 1) * rows)
            p = weights[i, part] * scale
            ds = p * (dprobs[i, part] - center)
            value_part = nn_dot(jnp.concatenate(split2(p), axis=1), grad_pair)
            s1, s2 = split2(ds)
            key_part = nn_dot(jnp.concatenate([s1, s2], axis=1), query_pair)
            query_part = nn_dot(key_t[b], jnp.concatenate([s1, s2], axis=0))
            query_sum = query_part if query_sum is None else query_sum + query_part
            if i == 0:
                value_acc[part] = value_part
                key_acc[part] = key_part
            else:
                value_acc[part] += value_part
                key_acc[part] += key_part
        query_t = (query_sum[:HEAD_DIM] + query_sum[HEAD_DIM:]) * SCORE_SCALE
        query_out[i][...] = query_t.T
    for b in range(nk):
        part = slice(b * rows, (b + 1) * rows)
        kv_out[b][0] = key_acc[part, :HEAD_DIM] + key_acc[part, HEAD_DIM:]
        kv_out[b][1] = value_acc[part, :HEAD_DIM] + value_acc[part, HEAD_DIM:]


def whole_vmem(count):
    return [pl.BlockSpec(memory_space=pltpu.VMEM)] * count


def partial_scores(bias, qd, kv, rows):
    nq, nk = len(qd), len(kv)
    big = jax.ShapeDtypeStruct((nq, nk * rows, rows), F32)
    return pl.pallas_call(
        functools.partial(score_kernel, nq, nk),
        out_shape=(big, big, jax.ShapeDtypeStruct((nq, 8, rows), F32)),
        in_specs=[pl.BlockSpec(memory_space=pltpu.SMEM)] + whole_vmem(nq + nk),
        out_specs=tuple(whole_vmem(3)),
        scratch_shapes=[
            pltpu.VMEM((nk * rows, 6 * HEAD_DIM), BF16),
            pltpu.VMEM((nk * rows, 4 * HEAD_DIM), BF16),
        ],
        name="scores",
    )(bias, *qd, *kv)


def partial_grads(weights, dprobs, coef, qd, kv, rows):
    nq, nk = len(qd), len(kv)
    outs = [jax.ShapeDtypeStruct((rows, HEAD_DIM), F32)] * nq
    outs += [jax.ShapeDtypeStruct((2, rows, HEAD_DIM), F32)] * nk
    result = pl.pallas_call(
        functools.partial(grad_kernel, nq, nk),
        out_shape=tuple(outs),
        in_specs=whole_vmem(3 + nq + nk),
        out_specs=tuple(whole_vmem(nq + nk)),
        scratch_shapes=[
            pltpu.VMEM((nk * rows, 2 * HEAD_DIM), F32),
            pltpu.VMEM((nk * rows, 2 * HEAD_DIM), F32),
            pltpu.VMEM((nk, 2 * HEAD_DIM, 2 * rows), BF16),
        ],
        name="grads",
    )(weights, dprobs, coef, *qd, *kv)
    return result[:nq], result[nq:]


def body(high, wide, query_field, key_field, value_field, output_grad):
    frames, rows_local, cols_local, channels = query_field.shape
    per_tile = TILE // cols_local
    pairs = per_tile // 2
    tiles = wide // per_tile
    rows_own = frames * rows_local * cols_local
    rows = 2 * rows_own
    around = high > 2

    def moved(value, dx, dy, dz):
        route = []
        for a in range(high):
            for w in range(wide):
                tile, pair, core = w // per_tile, (w % per_tile) // 2, w % 2
                to_a = a + dy if around else (a + dy) % high
                to_tile = tile + dz
                if 0 <= to_a < high and 0 <= to_tile < tiles:
                    to_w = to_tile * per_tile + ((pair + dx) % pairs) * 2 + core
                    route.append((a * wide + w, to_a * wide + to_w))
        return lax.ppermute(value, AXES, route)

    def swapped(value):
        route = [(a * wide + w, a * wide + (w ^ 1)) for a in range(high) for w in range(wide)]
        return lax.ppermute(value, AXES, route)

    row_steps = (0, -1, 1) if around else tuple(range(high))
    places = [(dx, dy) for dy in row_steps for dx in range(pairs)]
    nq = len(places)

    width_index = lax.axis_index("wa")
    head = width_index % 2
    tile = width_index // per_tile
    stacked = jnp.stack([query_field * SCORE_SCALE, output_grad, key_field, value_field])
    stacked = stacked.reshape(4, rows_own, channels)
    kept = lax.dynamic_slice_in_dim(stacked, head * HEAD_DIM, HEAD_DIM, 2)
    sent = lax.dynamic_slice_in_dim(stacked, (1 - head) * HEAD_DIM, HEAD_DIM, 2)
    received = swapped(sent)
    qd_own = jnp.stack([kept[:2], received[:2]])
    kv_own = jnp.stack([kept[2:], received[2:]])

    qd = [qd_own] + [moved(qd_own, -dx, -dy, 0) for dx, dy in places[1:]]
    sides = [0, -1, 1]
    kv = [kv_own] + [moved(kv_own, 0, 0, -dz) for dz in sides[1:]]
    at = tile + jnp.array(sides, jnp.int32)
    bias = jnp.where((at >= 0) & (at < tiles), 0.0, -1e30).astype(F32)

    weights, dprobs, stats = partial_scores(bias, qd, kv, rows)

    if around:
        parts = [stats[0]] + [moved(stats[i], dx, dy, 0) for i, (dx, dy) in enumerate(places) if i]
        parts = jnp.stack(parts)
        seen = parts[:, 1] > 0.0
        peak = jnp.max(jnp.where(seen, parts[:, 0], -jnp.inf), axis=0)
        factor = jnp.where(seen, jnp.exp(parts[:, 0] - peak), 0.0)
        total = jnp.sum(factor * parts[:, 1], axis=0)
        center = jnp.sum(factor * parts[:, 2], axis=0) / total
        final = jnp.stack([peak, total, center])
        final = jnp.stack([final] + [moved(final, -dx, -dy, 0) for dx, dy in places[1:]])
        peak, total, center = final[:, 0], final[:, 1], final[:, 2]
        inside = total > 0.0
        scale = jnp.where(inside, jnp.exp(stats[:, 0] - peak) / jnp.where(inside, total, 1.0), 0.0)
    else:
        spot = {place: i for i, place in enumerate(places)}
        parts = []
        for dx, dy in places:
            got = stats if (dx, dy) == (0, 0) else moved(stats, -dx, -dy, 0)
            order = [spot[((x - dx) % pairs, (y - dy) % high)] for x, y in places]
            parts.append(jnp.stack([got[j] for j in order]))
        parts = jnp.stack(parts)
        peak = jnp.max(parts[:, :, 0], axis=0)
        factor = jnp.exp(parts[:, :, 0] - peak)
        total = jnp.sum(factor * parts[:, :, 1], axis=0)
        center = jnp.sum(factor * parts[:, :, 2], axis=0) / total
        scale = factor[0] / total
    coef = jnp.stack([scale, center], axis=1)

    query_parts, kv_parts = partial_grads(weights, dprobs, coef, qd, kv, rows)

    kv_sum = kv_parts[0]
    for b, dz in enumerate(sides):
        if dz:
            kv_sum = kv_sum + moved(kv_parts[b], 0, 0, dz)
    query_sum = query_parts[0]
    for i, (dx, dy) in enumerate(places):
        if i:
            query_sum = query_sum + moved(query_parts[i], dx, dy, 0)

    summed = jnp.concatenate([query_sum[None], kv_sum]).reshape(3, 2, rows_own, HEAD_DIM)
    mine = summed[:, 0]
    other = swapped(summed[:, 1])
    first = head == 0
    result = jnp.concatenate([jnp.where(first, mine, other), jnp.where(first, other, mine)], axis=2)
    result = result.reshape(3, frames, rows_local, cols_local, channels)
    return result[0], result[1], result[2]


def solution(mesh):
    placed = P(None, "ha", "wa", None)
    return jax.shard_map(
        functools.partial(body, mesh.shape["ha"], mesh.shape["wa"]),
        mesh=mesh,
        in_specs=(placed,) * 4,
        out_specs=(placed,) * 3,
        check_vma=False,
    )
```

```python
import functools

import jax
import jax.numpy as jnp
from jax import lax
from jax.experimental import pallas as pl
from jax.experimental.pallas import tpu as pltpu
from jax.sharding import PartitionSpec as P

HEADS = 2
HEAD_DIM = 128
TILE = 16
AXES = ("ha", "wa")
SCORE_SCALE = HEAD_DIM ** (-0.5)
F32 = jnp.float32
BF16 = jnp.bfloat16


def split2(x):
    high = x.astype(BF16)
    return high, (x - high.astype(F32)).astype(BF16)


def split3(x):
    high = x.astype(BF16)
    rest = x - high.astype(F32)
    mid = rest.astype(BF16)
    return high, mid, (rest - mid.astype(F32)).astype(BF16)


def nt_dot(a, b):
    return lax.dot_general(a, b, (((1,), (1,)), ((), ())), preferred_element_type=F32)


def nn_dot(a, b):
    return lax.dot_general(a, b, (((1,), (0,)), ((), ())), preferred_element_type=F32)


def flat_rows(ref, part):
    block = ref[:, part]
    return block.reshape(-1, block.shape[-1])


def score_kernel(nq, nk, *refs):
    bias = refs[0]
    qd = refs[1 : 1 + nq]
    kv = refs[1 + nq : 1 + nq + nk]
    weights, dprobs, stats = refs[1 + nq + nk : 4 + nq + nk]
    key_cat, value_cat = refs[4 + nq + nk :]
    rows = weights.shape[1] // nk
    for b in range(nk):
        k1, k2, k3 = split3(flat_rows(kv[b], 0))
        key_cat[b * rows : (b + 1) * rows] = jnp.concatenate([k1, k1, k2, k2, k1, k3], axis=1)
        v1, v2 = split2(flat_rows(kv[b], 1))
        value_cat[b * rows : (b + 1) * rows] = jnp.concatenate([v1, v1, v2, v2], axis=1)
    for i in range(nq):
        q1, q2, q3 = split3(flat_rows(qd[i], 0))
        query_cat = jnp.concatenate([q1, q2, q1, q2, q3, q1], axis=1)
        d1, d2 = split2(flat_rows(qd[i], 1))
        grad_cat = jnp.concatenate([d1, d2, d1, d2], axis=1)
        peak = None
        for b in range(nk):
            part = slice(b * rows, (b + 1) * rows)
            scores = nt_dot(key_cat[part], query_cat) + bias[b]
            weights[i, part] = scores
            top = jnp.max(scores, axis=0, keepdims=True)
            peak = top if peak is None else jnp.maximum(peak, top)
        total = jnp.zeros_like(peak)
        center = jnp.zeros_like(peak)
        for b in range(nk):
            part = slice(b * rows, (b + 1) * rows)
            w = jnp.exp(weights[i, part] - peak)
            dp = nt_dot(value_cat[part], grad_cat)
            weights[i, part] = w
            dprobs[i, part] = dp
            total += jnp.sum(w, axis=0, keepdims=True)
            center += jnp.sum(w * dp, axis=0, keepdims=True)
        stats[i] = jnp.concatenate([peak, total, center, jnp.zeros((5, peak.shape[1]), F32)], axis=0)


def pack_kernel(head, query, grad, key, value, sent, kept):
    first = head[0] == 0
    for n, ref in enumerate((query, grad, key, value)):
        low = ref[..., :HEAD_DIM]
        high = ref[..., HEAD_DIM:]
        if n == 0:
            low, high = low * SCORE_SCALE, high * SCORE_SCALE
        kept[n] = jnp.where(first, low, high).reshape(-1, HEAD_DIM)
        sent[n] = jnp.where(first, high, low).reshape(-1, HEAD_DIM)


def unpack_kernel(head, mine, other, *outs):
    first = head[0] == 0
    for n, out in enumerate(outs):
        shape = out.shape[:-1] + (HEAD_DIM,)
        a, b = mine[n], other[n]
        out[..., :HEAD_DIM] = jnp.where(first, a, b).reshape(shape)
        out[..., HEAD_DIM:] = jnp.where(first, b, a).reshape(shape)


def grad_kernel(nq, nk, orders, *refs):
    weights, dprobs, stats = refs[:3]
    parts = refs[3 : 3 + len(orders)]
    refs = refs[3 + len(orders) :]
    qd = refs[:nq]
    kv = refs[nq : nq + nk]
    outs = refs[nq + nk :]
    query_out = outs[:nq]
    kv_out = outs[nq : nq + nk]
    key_acc, value_acc, key_t = outs[nq + nk :]
    rows = weights.shape[1] // nk
    for b in range(nk):
        k1, k2 = split2(flat_rows(kv[b], 0).T)
        both = jnp.concatenate([k1, k2], axis=0)
        key_t[b] = jnp.concatenate([both, both], axis=1)
    for i in range(nq):
        q1, q2 = split2(flat_rows(qd[i], 0))
        query_pair = jnp.concatenate([q1, q2], axis=1)
        query_pair = jnp.concatenate([query_pair, query_pair], axis=0)
        d1, d2 = split2(flat_rows(qd[i], 1))
        grad_pair = jnp.concatenate([d1, d2], axis=1)
        grad_pair = jnp.concatenate([grad_pair, grad_pair], axis=0)
        seen = [part[order[i]] for part, order in zip(parts, orders)]
        peak = functools.reduce(jnp.maximum, [x[0:1] for x in seen])
        factors = [jnp.exp(x[0:1] - peak) for x in seen]
        total = sum(f * x[1:2] for f, x in zip(factors, seen))
        total = jnp.where(total > 0.0, total, 1.0)
        center = sum(f * x[2:3] for f, x in zip(factors, seen)) / total
        scale = jnp.exp(stats[i, 0:1] - peak) / total
        query_sum = None
        for b in range(nk):
            part = slice(b * rows, (b + 1) * rows)
            p = weights[i, part] * scale
            ds = p * (dprobs[i, part] - center)
            value_part = nn_dot(jnp.concatenate(split2(p), axis=1), grad_pair)
            s1, s2 = split2(ds)
            key_part = nn_dot(jnp.concatenate([s1, s2], axis=1), query_pair)
            query_part = nn_dot(key_t[b], jnp.concatenate([s1, s2], axis=0))
            query_sum = query_part if query_sum is None else query_sum + query_part
            if i == 0:
                value_acc[part] = value_part
                key_acc[part] = key_part
            else:
                value_acc[part] += value_part
                key_acc[part] += key_part
        query_t = (query_sum[:HEAD_DIM] + query_sum[HEAD_DIM:]) * SCORE_SCALE
        query_out[i][...] = query_t.T
    for b in range(nk):
        part = slice(b * rows, (b + 1) * rows)
        kv_out[b][0] = key_acc[part, :HEAD_DIM] + key_acc[part, HEAD_DIM:]
        kv_out[b][1] = value_acc[part, :HEAD_DIM] + value_acc[part, HEAD_DIM:]


def run_kernel(kernel, name, args, outs, scratch=(), scalars=0, limit=24, keep=True):
    vmem = pl.BlockSpec(memory_space=pltpu.VMEM)
    smem = pl.BlockSpec(memory_space=pltpu.SMEM)
    if keep:
        args = [a if n < scalars else pltpu.with_memory_space_constraint(a, pltpu.VMEM) for n, a in enumerate(args)]
    return pl.pallas_call(
        kernel,
        out_shape=tuple(pltpu.VMEM(shape, F32) if vm else jax.ShapeDtypeStruct(shape, F32) for shape, vm in outs),
        in_specs=[smem] * scalars + [vmem] * (len(args) - scalars),
        out_specs=tuple([vmem] * len(outs)),
        scratch_shapes=list(scratch),
        compiler_params=pltpu.CompilerParams(vmem_limit_bytes=limit * 2**20),
        name=name,
    )(*args)


def partial_scores(bias, qd, kv, rows):
    nq, nk = len(qd), len(kv)
    big = ((nq, nk * rows, rows), True)
    return run_kernel(
        functools.partial(score_kernel, nq, nk),
        "scores",
        [bias, *qd, *kv],
        [big, big, ((nq, 8, rows), True)],
        [pltpu.VMEM((nk * rows, 6 * HEAD_DIM), BF16), pltpu.VMEM((nk * rows, 4 * HEAD_DIM), BF16)],
        scalars=1,
    )


def partial_grads(weights, dprobs, stats, parts, orders, qd, kv, rows):
    nq, nk = len(qd), len(kv)
    result = run_kernel(
        functools.partial(grad_kernel, nq, nk, orders),
        "grads",
        [weights, dprobs, stats, *parts, *qd, *kv],
        [((rows, HEAD_DIM), True)] * nq + [((2, rows, HEAD_DIM), True)] * nk,
        [
            pltpu.VMEM((nk * rows, 2 * HEAD_DIM), F32),
            pltpu.VMEM((nk * rows, 2 * HEAD_DIM), F32),
            pltpu.VMEM((nk, 2 * HEAD_DIM, 2 * rows), BF16),
        ],
    )
    return result[:nq], result[nq:]


def body(high, wide, query_field, key_field, value_field, output_grad):
    frames, rows_local, cols_local, channels = query_field.shape
    per_tile = TILE // cols_local
    pairs = per_tile // 2
    tiles = wide // per_tile
    rows_own = frames * rows_local * cols_local
    rows = 2 * rows_own
    around = high > 2

    def moved(value, dx, dy, dz):
        route = []
        for a in range(high):
            for w in range(wide):
                tile, pair, core = w // per_tile, (w % per_tile) // 2, w % 2
                to_a = a + dy if around else (a + dy) % high
                to_tile = tile + dz
                if 0 <= to_a < high and 0 <= to_tile < tiles:
                    to_w = to_tile * per_tile + ((pair + dx) % pairs) * 2 + core
                    route.append((a * wide + w, to_a * wide + to_w))
        return lax.ppermute(value, AXES, route)

    def swapped(value):
        route = [(a * wide + w, a * wide + (w ^ 1)) for a in range(high) for w in range(wide)]
        return lax.ppermute(value, AXES, route)

    row_steps = (0, -1, 1) if around else tuple(range(high))
    places = [(dx, dy) for dy in row_steps for dx in range(pairs)]
    nq = len(places)

    width_index = lax.axis_index("wa")
    head = width_index % 2
    tile = width_index // per_tile
    head_cell = head.astype(jnp.int32).reshape(1)
    small = ((4, rows_own, HEAD_DIM), True)
    sent, kept = run_kernel(
        pack_kernel, "pack", [head_cell, query_field, output_grad, key_field, value_field], [small, small], scalars=1, keep=False
    )
    received = swapped(sent)
    qd_own = jnp.stack([kept[:2], received[:2]])
    kv_own = jnp.stack([kept[2:], received[2:]])

    qd = [qd_own] + [moved(qd_own, -dx, -dy, 0) for dx, dy in places[1:]]
    sides = [0, -1, 1]
    kv = [kv_own] + [moved(kv_own, 0, 0, -dz) for dz in sides[1:]]
    at = tile + jnp.array(sides, jnp.int32)
    bias = jnp.where((at >= 0) & (at < tiles), 0.0, -1e30).astype(F32)

    weights, dprobs, stats = partial_scores(bias, qd, kv, rows)

    if around:
        parts = [stats[0]] + [moved(stats[i], dx, dy, 0) for i, (dx, dy) in enumerate(places) if i]
        parts = jnp.stack(parts)
        seen = parts[:, 1] > 0.0
        peak = jnp.max(jnp.where(seen, parts[:, 0], -jnp.inf), axis=0)
        factor = jnp.where(seen, jnp.exp(parts[:, 0] - peak), 0.0)
        total = jnp.sum(factor * parts[:, 1], axis=0)
        center = jnp.sum(factor * parts[:, 2], axis=0)
        final = jnp.stack([peak, total, center] + [jnp.zeros_like(peak)] * 5)
        final = jnp.stack([final] + [moved(final, -dx, -dy, 0) for dx, dy in places[1:]])
        parts, orders = [final], [list(range(nq))]
    else:
        spot = {place: i for i, place in enumerate(places)}
        parts = [stats] + [moved(stats, -dx, -dy, 0) for dx, dy in places[1:]]
        orders = [[spot[((x - dx) % pairs, (y - dy) % high)] for x, y in places] for dx, dy in places]

    query_parts, kv_parts = partial_grads(weights, dprobs, stats, parts, orders, qd, kv, rows)

    kv_sum = kv_parts[0]
    for b, dz in enumerate(sides):
        if dz:
            kv_sum = kv_sum + moved(kv_parts[b], 0, 0, dz)
    query_sum = query_parts[0]
    for i, (dx, dy) in enumerate(places):
        if i:
            query_sum = query_sum + moved(query_parts[i], dx, dy, 0)

    summed = jnp.concatenate([query_sum[None], kv_sum]).reshape(3, 2, rows_own, HEAD_DIM)
    mine = summed[:, 0]
    other = swapped(summed[:, 1])
    shape = (frames, rows_local, cols_local, channels)
    return run_kernel(unpack_kernel, "unpack", [head_cell, mine, other], [(shape, False)] * 3, scalars=1)


def solution(mesh):
    placed = P(None, "ha", "wa", None)
    return jax.shard_map(
        functools.partial(body, mesh.shape["ha"], mesh.shape["wa"]),
        mesh=mesh,
        in_specs=(placed,) * 4,
        out_specs=(placed,) * 3,
        check_vma=False,
    )
```
